32 devices in a mesh: gx: 4 (over y, x), gy: 4 (over z), gz: 2 (over core).
Axes of the slice: x: 2, y: 2, z: 4, core: 2. Of those that a mesh axis runs over, the one named last changes fastest.
Arguments:
- material: int32 [128, 256, 256], P('gx', 'gy', 'gz'), may hold values from 0 to 7
- eps_table: float32 [8], replicated, may hold values from 1 to 13
- grading: bfloat16 [128, 256, 256], P('gx', 'gy', 'gz'), may hold values from 0.25 to 1.75
Outputs:
- smoothed: bfloat16 [6, 128, 256, 256], P(None, 'gx', 'gy', 'gz')
The draws below stay inside these ranges and needn't reach their ends.
All inputs are finite; a program needn't handle non-finite values.
Results may differ from the reference program's by a relative error of at most 0.001.
Values sent between devices are 32-bit elements; how exact they have to be, the bound alone decides.
A program may use at most 64 MiB of HBM per device.

```python
import math
import jax
import jax.numpy as jnp

MATERIALS = 8
NX = 128
NY = 256
NZ = 256


def touch_ends(drawn, rng, low, top_value):
    dims = drawn.shape
    spot = [jax.random.randint(jax.random.fold_in(rng, axis), (), 0, dims[axis]) for axis in range(len(dims))]
    drawn = drawn.at[tuple(spot)].set(low)
    longest = dims.index(max(dims))
    spot[longest] = (spot[longest] + 1) % dims[longest]
    return drawn.at[tuple(spot)].set(top_value)


def setup_inputs(seed: int = 0) -> dict:
    seeds = jax.random.split(jax.random.key(seed), 4)
    return {
        "material": touch_ends(jax.random.randint(seeds[0], (NX, NY, NZ), 0, MATERIALS), jax.random.fold_in(seeds[0], 1), 0, MATERIALS - 1).astype(jnp.int32),
        "eps_table": jnp.clip(jnp.exp(jax.random.uniform(seeds[1], (MATERIALS,), jnp.float32, math.log(1.0), math.log(13.0))), 1.0, 13.0),
        "grading": jnp.clip(1.0 + 0.15 * jax.random.normal(seeds[2], (NX, NY, NZ), jnp.float32), 0.25, 1.75).astype(jnp.bfloat16),
    }


def lookup(material, eps_table, grading):
    values = jnp.zeros(material.shape, jnp.float32)
    for index in range(eps_table.shape[0]):
        values = jnp.where(material == index, eps_table[index], values)
    return values * grading.astype(jnp.float32)


def box_mean(padded):
    total = padded[:-2] + padded[1:-1] + padded[2:]
    total = total[:, :-2] + total[:, 1:-1] + total[:, 2:]
    total = total[:, :, :-2] + total[:, :, 1:-1] + total[:, :, 2:]
    return total / 27.0


def tensor(mean_ext, mean_inv):
    centre = mean_ext[1:-1, 1:-1, 1:-1]
    grad_x = (mean_ext[2:, 1:-1, 1:-1] - mean_ext[:-2, 1:-1, 1:-1]) * 0.5
    grad_y = (mean_ext[1:-1, 2:, 1:-1] - mean_ext[1:-1, :-2, 1:-1]) * 0.5
    grad_z = (mean_ext[1:-1, 1:-1, 2:] - mean_ext[1:-1, 1:-1, :-2]) * 0.5
    scale = 1.0 / (grad_x * grad_x + grad_y * grad_y + grad_z * grad_z + 0.1)
    recip = 1.0 / centre
    grads = (grad_x, grad_y, grad_z)
    pairs = ((0, 0), (1, 1), (2, 2), (0, 1), (0, 2), (1, 2))
    result = []
    for first, second in pairs:
        weight = grads[first] * grads[second] * scale
        delta = 1.0 if first == second else 0.0
        result.append(mean_inv * weight + (delta - weight) * recip)
    return jnp.stack(result, 0).astype(jnp.bfloat16)


def reference(material, eps_table, grading):
    eps = lookup(material, eps_table, grading)
    padded = jnp.pad(eps, 2, mode="wrap")
    mean_ext = box_mean(padded)
    mean_inv = box_mean(1.0 / padded)[1:-1, 1:-1, 1:-1]
    return tensor(mean_ext, mean_inv)
```

```python
import functools

import jax
import jax.numpy as jnp
from jax import lax
from jax.experimental import pallas as pl
from jax.experimental.pallas import tpu as pltpu
from jax.sharding import PartitionSpec as P

MESH = pl.DeviceIdType.MESH
CHUNKS = 4
PAD = 8


def inverse(x):
    guess = pl.reciprocal(x, approx=True)
    return guess * (2.0 - x * guess)


def kernel(nx, ny, nz, X, Y, mat_hbm, table, grad_hbm, out, mat, grad, eps, peer, halo, halo_peer, faces,
           zs, zd, zi, in_sem, main_send, main_recv, face_send, face_recv, fwd_send, fwd_recv):
    Z = mat.shape[-1]
    zpeers = 1 if nz == 2 else 2
    xs, ys = 2 * Y, 2 * X
    pieces = ((0, xs), (xs, xs), (2 * xs, ys), (2 * xs + ys, ys)) + tuple(
        (2 * xs + 2 * ys + 8 * c, 8) for c in range(4)
    )
    rows = X * Y // CHUNKS

    def load(c):
        part = pl.ds(c * rows, rows)
        return (
            pltpu.make_async_copy(mat_hbm.at[part], mat.at[part], in_sem.at[0, c]),
            pltpu.make_async_copy(grad_hbm.at[part], grad.at[part], in_sem.at[1, c]),
        )

    order = (0, CHUNKS - 1) + tuple(range(1, CHUNKS - 1))
    for c in order:
        for copy in load(c):
            copy.start()

    me = (lax.axis_index("gx"), lax.axis_index("gy"), lax.axis_index("gz"))
    sizes = (nx, ny, nz)

    def near(*steps):
        return tuple(
            me[k] if d == 0 else lax.rem(me[k] + (d + sizes[k]), sizes[k]) for k, d in enumerate(steps)
        )

    zdevs = [near(0, 0, 1), near(0, 0, -1)][:zpeers]
    around = [near(i, j, 0) for i in (-1, 0, 1) for j in (-1, 0, 1) if (i, j) != (0, 0)]
    barrier = pltpu.get_barrier_semaphore()
    for dev in around + zdevs:
        pl.semaphore_signal(barrier, inc=1, device_id=dev, device_id_type=MESH)

    values = [table[k] for k in range(table.shape[0])]

    def look(c):
        for copy in load(c):
            copy.wait()

        def plane(i, carry):
            part = pl.ds(pl.multiple_of(c * rows + i * Y, Y), Y)
            m = mat[part]
            v = jnp.full(m.shape, values[0], jnp.float32)
            for k in range(1, len(values)):
                v = jnp.where(m == k, values[k], v)
            eps[part] = v * grad[part].astype(jnp.float32)
            return carry

        lax.fori_loop(0, rows // Y, plane, 0)

    def main_copy(c, side):
        part = pl.ds(c * rows, rows)
        return pltpu.make_async_remote_copy(
            eps.at[part], peer.at[side, part], main_send.at[side, c], main_recv.at[side, c],
            device_id=zdevs[side], device_id_type=MESH,
        )

    def piece(ref, k):
        return ref.at[pl.ds(pieces[k][0], pieces[k][1])]

    def face_copy(k, src, dev):
        return pltpu.make_async_remote_copy(
            src, piece(halo, k), face_send.at[k], face_recv.at[k], device_id=dev, device_id_type=MESH
        )

    def forward(k, side):
        start, count = pieces[k]
        return pltpu.make_async_remote_copy(
            piece(halo, k), halo_peer.at[side, pl.ds(start, count)], fwd_send.at[side, k],
            fwd_recv.at[side, k], device_id=zdevs[side], device_id_type=MESH,
        )

    edges = 2 * ys
    copies = {
        1: face_copy(1, eps.at[pl.ds(0, xs)], near(-1, 0, 0)),
        0: face_copy(0, eps.at[pl.ds(X * Y - xs, xs)], near(1, 0, 0)),
        3: face_copy(3, faces.at[pl.ds(0, ys)], near(0, -1, 0)),
        2: face_copy(2, faces.at[pl.ds(ys, ys)], near(0, 1, 0)),
    }
    for sx in range(2):
        for sy in range(2):
            mine, theirs = 2 * sx + sy, 2 * (1 - sx) + (1 - sy)
            copies[4 + theirs] = face_copy(
                4 + theirs, faces.at[pl.ds(edges + 8 * mine, 8)], near(2 * sx - 1, 2 * sy - 1, 0)
            )
    mains = {(c, s): main_copy(c, s) for c in order for s in range(zpeers)}
    forwards = {(k, s): forward(k, s) for k in range(8) for s in range(zpeers)}

    for c in order[:2]:
        look(c)
    pl.semaphore_wait(barrier, len(around) + len(zdevs))
    copies[0].start()
    copies[1].start()
    for c in order[2:]:
        look(c)
    for l in range(2):
        for side in range(2):
            y = l if side == 0 else Y - 2 + l
            faces[pl.ds(side * ys + l * X, X)] = eps[pl.ds(y, X, stride=Y)]
    faces[pl.ds(edges, 32)] = jnp.ones((32, Z), jnp.float32)
    for sx in range(2):
        for sy in range(2):
            for a in range(2):
                x, y = (X - 2) * sx + a, (Y - 2) * sy
                faces[pl.ds(edges + 8 * (2 * sx + sy) + 2 * a, 2)] = eps[pl.ds(x * Y + y, 2)]
    for c in order:
        for s in range(zpeers):
            mains[c, s].start()
    for k in range(4, 8):
        copies[k].start()
    for k in (2, 3):
        copies[k].start()

    def zfilter(e, low, high):
        lane = lax.broadcasted_iota(jnp.int32, e.shape, 1)
        m1 = pltpu.roll(jnp.where(lane == Z - 1, low, e), 1, 1)
        m2 = pltpu.roll(jnp.where(lane >= Z - 2, low, e), 2, 1)
        p1 = pltpu.roll(jnp.where(lane == 0, high, e), Z - 1, 1)
        p2 = pltpu.roll(jnp.where(lane < 2, high, e), Z - 2, 1)
        both, prod = m1 + p1, m1 * p1
        return e + both, (p1 - m1) + (p2 - m2), (prod + e * both) * inverse(e * prod)

    def sides(ref, part):
        low = ref[0, part]
        return low, (low if zpeers == 1 else ref[1, part])

    for c in order:
        for s in range(zpeers):
            mains[c, s].wait_recv()

        def plane(i, carry):
            x = c * (rows // Y) + i
            part = pl.ds(pl.multiple_of(x * Y, Y), Y)
            for ref, value in zip((zs, zd, zi), zfilter(eps[part], *sides(peer, part))):
                ref[x + 2, PAD:PAD + Y] = value
            return carry

        lax.fori_loop(0, rows // Y, plane, 0)

    def yrows(ref, p, j, shift):
        return ref[p, PAD + 16 * j + shift:PAD + 16 * j + shift + 16]

    def lead(p, j):
        a, b = yrows(zs, p, j, -1), yrows(zs, p, j, 1)
        return yrows(zs, p, j, 0) + (a + b)

    def rest(p, j):
        b = (yrows(zs, p, j, 1) - yrows(zs, p, j, -1)) + (yrows(zs, p, j, 2) - yrows(zs, p, j, -2))
        return b, sum(yrows(zd, p, j, k) for k in (-1, 0, 1)), sum(yrows(zi, p, j, k) for k in (-1, 0, 1))

    def outputs(j, start, count, unroll):
        def step(x, carry):
            (a0, a1, a2, a3), r0, r1 = carry
            a4 = lead(x + 4, j)
            r2 = rest(x + 3, j)
            total = a2 + (a1 + a3)
            gx = (a3 - a1) + (a4 - a0)
            gy, gz, inv = (u + v + w for u, v, w in zip(r0, r1, r2))
            den = gx * gx + gy * gy + gz * gz + 291.6
            q = inverse(total * den)
            recip = (den * q) * 27.0
            k = (inv * (1.0 / 27.0) - recip) * (total * q)
            kx, ky, kz = gx * k, gy * k, gz * k
            result = (gx * kx + recip, gy * ky + recip, gz * kz + recip, gx * ky, gx * kz, gy * kz)
            for n, value in enumerate(result):
                out[n, x, 16 * j:16 * j + 16] = value.astype(out.dtype)
            return (a1, a2, a3, a4), r1, r2

        carry = (tuple(lead(start + k, j) for k in range(4)), rest(start + 1, j), rest(start + 2, j))
        if count == unroll:
            for k in range(count):
                carry = step(start + k, carry)
        else:
            def block(i, carry):
                for k in range(unroll):
                    carry = step(start + i * unroll + k, carry)
                return carry

            lax.fori_loop(0, count // unroll, block, carry)

    def arrive(ks):
        for k in ks:
            copies[k].wait_recv()
            for s in range(zpeers):
                forwards[k, s].start()

    def halo_filter(k):
        for s in range(zpeers):
            forwards[k, s].wait_recv()
        part = pl.ds(*pieces[k])
        fields = zfilter(halo[part], *sides(halo_peer, part))
        for ref, value in zip((zs, zd, zi), fields):
            if k < 2:
                p = k * (X + 2)
                ref[p, PAD:PAD + Y] = value[:Y]
                ref[p + 1, PAD:PAD + Y] = value[Y:]
            elif k < 4:
                flat = ref.reshape((X + 4) * (Y + 2 * PAD), Z)
                y = PAD - 2 if k == 2 else PAD + Y
                for l in range(2):
                    flat[pl.ds(2 * (Y + 2 * PAD) + y + l, X, stride=Y + 2 * PAD)] = value[l * X:(l + 1) * X]
            else:
                sx, sy = divmod(k - 4, 2)
                y = PAD - 2 if sy == 0 else PAD + Y
                for a in range(2):
                    ref[sx * (X + 2) + a, y:y + 2] = value[2 * a:2 * a + 2]

    pairs = Y // 16
    unroll = 4
    inside = range(1, pairs - 1)
    for n, j in enumerate(inside):
        outputs(j, 2, X - 4, unroll)
        if n == 0:
            arrive((2, 3))
    arrive((0, 1, 4, 5, 6, 7))
    halo_filter(2)
    halo_filter(3)
    outputs(0, 2, X - 4, unroll)
    outputs(pairs - 1, 2, X - 4, unroll)
    for k in (0, 1, 4, 5, 6, 7):
        halo_filter(k)
    for j in range(pairs):
        outputs(j, 0, 2, 2)
        outputs(j, X - 2, 2, 2)
    for copy in list(copies.values()) + list(mains.values()) + list(forwards.values()):
        copy.wait_send()


def solution(mesh):
    nx, ny, nz = mesh.shape["gx"], mesh.shape["gy"], mesh.shape["gz"]

    def local(material, eps_table, grading):
        X, Y, Z = material.shape
        zpeers = 1 if nz == 2 else 2
        halo_rows = 4 * Y + 4 * X + 32
        any_space = pl.BlockSpec(memory_space=pl.ANY)
        dma = pltpu.SemaphoreType.DMA
        field = pltpu.VMEM((X + 4, Y + 2 * PAD, Z), jnp.float32)
        return pl.pallas_call(
            functools.partial(kernel, nx, ny, nz, X, Y),
            out_shape=jax.ShapeDtypeStruct((6, X, Y, Z), jnp.bfloat16),
            in_specs=[any_space, pl.BlockSpec(memory_space=pltpu.SMEM), any_space],
            out_specs=pl.BlockSpec(memory_space=pltpu.VMEM),
            scratch_shapes=[
                pltpu.VMEM((X * Y, Z), jnp.int32),
                pltpu.VMEM((X * Y, Z), jnp.bfloat16),
                pltpu.VMEM((X * Y, Z), jnp.float32),
                pltpu.VMEM((zpeers, X * Y, Z), jnp.float32),
                pltpu.VMEM((halo_rows, Z), jnp.float32),
                pltpu.VMEM((zpeers, halo_rows, Z), jnp.float32),
                pltpu.VMEM((4 * X + 32, Z), jnp.float32),
                field, field, field,
                dma((2, CHUNKS)),
                dma((zpeers, CHUNKS)), dma((zpeers, CHUNKS)),
                dma((8,)), dma((8,)),
                dma((zpeers, 8)), dma((zpeers, 8)),
            ],
            compiler_params=pltpu.CompilerParams(collective_id=0, has_side_effects=True),
        )(material.reshape(X * Y, Z), eps_table, grading.reshape(X * Y, Z))

    return jax.shard_map(
        local,
        mesh=mesh,
        in_specs=(P("gx", "gy", "gz"), P(), P("gx", "gy", "gz")),
        out_specs=P(None, "gx", "gy", "gz"),
        check_vma=False,
    )
```

```python
import functools

import jax
import jax.numpy as jnp
from jax import lax
from jax.experimental import pallas as pl
from jax.experimental.pallas import tpu as pltpu
from jax.sharding import PartitionSpec as P

MESH = pl.DeviceIdType.MESH
CHUNKS = 4
PAD = 8


def inverse(x):
    guess = pl.reciprocal(x, approx=True)
    return guess * (2.0 - x * guess)


def kernel(nx, ny, nz, X, Y, mat_hbm, table_hbm, grad_hbm, out, mat, table, grad, eps, peer, halo, halo_peer, faces,
           zs, zd, zi, in_sem, table_sem, main_send, main_recv, face_send, face_recv, fwd_send, fwd_recv):
    Z = mat.shape[-1]
    zpeers = 1 if nz == 2 else 2
    xs, ys = 2 * Y, 2 * X
    pieces = ((0, xs), (xs, xs), (2 * xs, ys), (2 * xs + ys, ys)) + tuple(
        (2 * xs + 2 * ys + 8 * c, 8) for c in range(4)
    )
    rows = X * Y // CHUNKS

    def load(c):
        part = pl.ds(c * rows, rows)
        return (
            pltpu.make_async_copy(mat_hbm.at[part], mat.at[part], in_sem.at[0, c]),
            pltpu.make_async_copy(grad_hbm.at[part], grad.at[part], in_sem.at[1, c]),
        )

    order = (0, CHUNKS - 1) + tuple(range(1, CHUNKS - 1))
    table_copy = pltpu.make_async_copy(table_hbm, table, table_sem)
    table_copy.start()
    for c in order:
        for copy in load(c):
            copy.start()

    me = (lax.axis_index("gx"), lax.axis_index("gy"), lax.axis_index("gz"))
    sizes = (nx, ny, nz)

    def near(*steps):
        return tuple(
            me[k] if d == 0 else lax.rem(me[k] + (d + sizes[k]), sizes[k]) for k, d in enumerate(steps)
        )

    zdevs = [near(0, 0, 1), near(0, 0, -1)][:zpeers]
    around = [near(i, j, 0) for i in (-1, 0, 1) for j in (-1, 0, 1) if (i, j) != (0, 0)]
    barrier = pltpu.get_barrier_semaphore()
    for dev in around + zdevs:
        pl.semaphore_signal(barrier, inc=1, device_id=dev, device_id_type=MESH)

    table_copy.wait()
    values = [table[k] for k in range(table.shape[0])]

    def look(c):
        for copy in load(c):
            copy.wait()

        def plane(i, carry):
            part = pl.ds(pl.multiple_of(c * rows + i * Y, Y), Y)
            m = mat[part]
            v = jnp.full(m.shape, values[0], jnp.float32)
            for k in range(1, len(values)):
                v = jnp.where(m == k, values[k], v)
            eps[part] = v * grad[part].astype(jnp.float32)
            return carry

        lax.fori_loop(0, rows // Y, plane, 0)

    def main_copy(c, side):
        part = pl.ds(c * rows, rows)
        return pltpu.make_async_remote_copy(
            eps.at[part], peer.at[side, part], main_send.at[side, c], main_recv.at[side, c],
            device_id=zdevs[side], device_id_type=MESH,
        )

    def piece(ref, k):
        return ref.at[pl.ds(pieces[k][0], pieces[k][1])]

    def face_copy(k, src, dev):
        return pltpu.make_async_remote_copy(
            src, piece(halo, k), face_send.at[k], face_recv.at[k], device_id=dev, device_id_type=MESH
        )

    def forward(k, side):
        start, count = pieces[k]
        return pltpu.make_async_remote_copy(
            piece(halo, k), halo_peer.at[side, pl.ds(start, count)], fwd_send.at[side, k],
            fwd_recv.at[side, k], device_id=zdevs[side], device_id_type=MESH,
        )

    edges = 2 * ys
    copies = {
        1: face_copy(1, eps.at[pl.ds(0, xs)], near(-1, 0, 0)),
        0: face_copy(0, eps.at[pl.ds(X * Y - xs, xs)], near(1, 0, 0)),
        3: face_copy(3, faces.at[pl.ds(0, ys)], near(0, -1, 0)),
        2: face_copy(2, faces.at[pl.ds(ys, ys)], near(0, 1, 0)),
    }
    for sx in range(2):
        for sy in range(2):
            mine, theirs = 2 * sx + sy, 2 * (1 - sx) + (1 - sy)
            copies[4 + theirs] = face_copy(
                4 + theirs, faces.at[pl.ds(edges + 8 * mine, 8)], near(2 * sx - 1, 2 * sy - 1, 0)
            )
    mains = {(c, s): main_copy(c, s) for c in order for s in range(zpeers)}
    forwards = {(k, s): forward(k, s) for k in range(8) for s in range(zpeers)}

    for c in order[:2]:
        look(c)
    pl.semaphore_wait(barrier, len(around) + len(zdevs))
    copies[0].start()
    copies[1].start()
    for c in order[2:]:
        look(c)
    for l in range(2):
        for side in range(2):
            y = l if side == 0 else Y - 2 + l
            faces[pl.ds(side * ys + l * X, X)] = eps[pl.ds(y, X, stride=Y)]
    faces[pl.ds(edges, 32)] = jnp.ones((32, Z), jnp.float32)
    for sx in range(2):
        for sy in range(2):
            for a in range(2):
                x, y = (X - 2) * sx + a, (Y - 2) * sy
                faces[pl.ds(edges + 8 * (2 * sx + sy) + 2 * a, 2)] = eps[pl.ds(x * Y + y, 2)]
    for c in order:
        for s in range(zpeers):
            mains[c, s].start()
    for k in range(4, 8):
        copies[k].start()
    for k in (2, 3):
        copies[k].start()

    def zfilter(e, low, high):
        lane = lax.broadcasted_iota(jnp.int32, e.shape, 1)
        m1 = pltpu.roll(jnp.where(lane == Z - 1, low, e), 1, 1)
        m2 = pltpu.roll(jnp.where(lane >= Z - 2, low, e), 2, 1)
        p1 = pltpu.roll(jnp.where(lane == 0, high, e), Z - 1, 1)
        p2 = pltpu.roll(jnp.where(lane < 2, high, e), Z - 2, 1)
        both, prod = m1 + p1, m1 * p1
        return e + both, (p1 - m1) + (p2 - m2), (prod + e * both) * inverse(e * prod)

    def sides(ref, part):
        low = ref[0, part]
        return low, (low if zpeers == 1 else ref[1, part])

    for c in order:
        for s in range(zpeers):
            mains[c, s].wait_recv()

        def plane(i, carry):
            x = c * (rows // Y) + i
            part = pl.ds(pl.multiple_of(x * Y, Y), Y)
            for ref, value in zip((zs, zd, zi), zfilter(eps[part], *sides(peer, part))):
                ref[x + 2, PAD:PAD + Y] = value
            return carry

        lax.fori_loop(0, rows // Y, plane, 0)

    def yrows(ref, p, j, shift):
        return ref[p, PAD + 16 * j + shift:PAD + 16 * j + shift + 16]

    def lead(p, j):
        a, b = yrows(zs, p, j, -1), yrows(zs, p, j, 1)
        return yrows(zs, p, j, 0) + (a + b)

    def rest(p, j):
        b = (yrows(zs, p, j, 1) - yrows(zs, p, j, -1)) + (yrows(zs, p, j, 2) - yrows(zs, p, j, -2))
        return b, sum(yrows(zd, p, j, k) for k in (-1, 0, 1)), sum(yrows(zi, p, j, k) for k in (-1, 0, 1))

    def outputs(j, start, count, unroll):
        def step(x, carry):
            (a0, a1, a2, a3), r0, r1 = carry
            a4 = lead(x + 4, j)
            r2 = rest(x + 3, j)
            total = a2 + (a1 + a3)
            gx = (a3 - a1) + (a4 - a0)
            gy, gz, inv = (u + v + w for u, v, w in zip(r0, r1, r2))
            den = gx * gx + gy * gy + gz * gz + 291.6
            q = inverse(total * den)
            recip = (den * q) * 27.0
            k = (inv * (1.0 / 27.0) - recip) * (total * q)
            kx, ky, kz = gx * k, gy * k, gz * k
            result = (gx * kx + recip, gy * ky + recip, gz * kz + recip, gx * ky, gx * kz, gy * kz)
            for n, value in enumerate(result):
                out[n, x, 16 * j:16 * j + 16] = value.astype(out.dtype)
            return (a1, a2, a3, a4), r1, r2

        carry = (tuple(lead(start + k, j) for k in range(4)), rest(start + 1, j), rest(start + 2, j))
        if count == unroll:
            for k in range(count):
                carry = step(start + k, carry)
        else:
            def block(i, carry):
                for k in range(unroll):
                    carry = step(start + i * unroll + k, carry)
                return carry

            lax.fori_loop(0, count // unroll, block, carry)

    def arrive(ks):
        for k in ks:
            copies[k].wait_recv()
            for s in range(zpeers):
                forwards[k, s].start()

    def halo_filter(k):
        for s in range(zpeers):
            forwards[k, s].wait_recv()
        part = pl.ds(*pieces[k])
        fields = zfilter(halo[part], *sides(halo_peer, part))
        for ref, value in zip((zs, zd, zi), fields):
            if k < 2:
                p = k * (X + 2)
                ref[p, PAD:PAD + Y] = value[:Y]
                ref[p + 1, PAD:PAD + Y] = value[Y:]
            elif k < 4:
                flat = ref.reshape((X + 4) * (Y + 2 * PAD), Z)
                y = PAD - 2 if k == 2 else PAD + Y
                for l in range(2):
                    flat[pl.ds(2 * (Y + 2 * PAD) + y + l, X, stride=Y + 2 * PAD)] = value[l * X:(l + 1) * X]
            else:
                sx, sy = divmod(k - 4, 2)
                y = PAD - 2 if sy == 0 else PAD + Y
                for a in range(2):
                    ref[sx * (X + 2) + a, y:y + 2] = value[2 * a:2 * a + 2]

    pairs = Y // 16
    unroll = 4
    inside = range(1, pairs - 1)
    for n, j in enumerate(inside):
        outputs(j, 2, X - 4, unroll)
        if n == 0:
            arrive((2, 3))
    arrive((0, 1, 4, 5, 6, 7))
    halo_filter(2)
    halo_filter(3)
    outputs(0, 2, X - 4, unroll)
    outputs(pairs - 1, 2, X - 4, unroll)
    for k in (0, 1, 4, 5, 6, 7):
        halo_filter(k)
    for j in range(pairs):
        outputs(j, 0, 2, 2)
        outputs(j, X - 2, 2, 2)
    for copy in list(copies.values()) + list(mains.values()) + list(forwards.values()):
        copy.wait_send()


def write_out(result, out, sem):
    copies = [pltpu.make_async_copy(result.at[n], out.at[n], sem.at[n]) for n in range(out.shape[0])]
    for copy in copies:
        copy.start()
    for copy in copies:
        copy.wait()


def solution(mesh):
    nx, ny, nz = mesh.shape["gx"], mesh.shape["gy"], mesh.shape["gz"]

    def local(material, eps_table, grading):
        X, Y, Z = material.shape
        zpeers = 1 if nz == 2 else 2
        halo_rows = 4 * Y + 4 * X + 32
        any_space = pl.BlockSpec(memory_space=pl.ANY)
        dma = pltpu.SemaphoreType.DMA
        field = pltpu.VMEM((X + 4, Y + 2 * PAD, Z), jnp.float32)
        result = pl.pallas_call(
            functools.partial(kernel, nx, ny, nz, X, Y),
            out_shape=pltpu.VMEM((6, X, Y, Z), jnp.bfloat16),
            in_specs=[pl.BlockSpec(memory_space=pltpu.HBM)] * 3,
            out_specs=pl.BlockSpec(memory_space=pltpu.VMEM),
            scratch_shapes=[
                pltpu.VMEM((X * Y, Z), jnp.int32),
                pltpu.SMEM(eps_table.shape, jnp.float32),
                pltpu.VMEM((X * Y, Z), jnp.bfloat16),
                pltpu.VMEM((X * Y, Z), jnp.float32),
                pltpu.VMEM((zpeers, X * Y, Z), jnp.float32),
                pltpu.VMEM((halo_rows, Z), jnp.float32),
                pltpu.VMEM((zpeers, halo_rows, Z), jnp.float32),
                pltpu.VMEM((4 * X + 32, Z), jnp.float32),
                field, field, field,
                dma((2, CHUNKS)), dma(()),
                dma((zpeers, CHUNKS)), dma((zpeers, CHUNKS)),
                dma((8,)), dma((8,)),
                dma((zpeers, 8)), dma((zpeers, 8)),
            ],
            compiler_params=pltpu.CompilerParams(
                collective_id=0, has_side_effects=True, vmem_limit_bytes=24 * 2**20
            ),
        )(*(pltpu.with_memory_space_constraint(a, pltpu.HBM)
            for a in (material.reshape(X * Y, Z), eps_table, grading.reshape(X * Y, Z))))
        return pl.pallas_call(
            write_out,
            out_shape=jax.ShapeDtypeStruct((6, X, Y, Z), jnp.bfloat16),
            in_specs=[pl.BlockSpec(memory_space=pltpu.VMEM)],
            out_specs=any_space,
            scratch_shapes=[dma((6,))],
            compiler_params=pltpu.CompilerParams(vmem_limit_bytes=24 * 2**20),
        )(result)

    return jax.shard_map(
        local,
        mesh=mesh,
        in_specs=(P("gx", "gy", "gz"), P(), P("gx", "gy", "gz")),
        out_specs=P(None, "gx", "gy", "gz"),
        check_vma=False,
    )
```

```python
import functools

import jax
import jax.numpy as jnp
from jax import lax
from jax.experimental import pallas as pl
from jax.experimental.pallas import tpu as pltpu
from jax.sharding import PartitionSpec as P

MESH = pl.DeviceIdType.MESH
CHUNKS = 4
PAD = 8


def inverse(x):
    guess = pl.reciprocal(x, approx=True)
    return guess * (2.0 - x * guess)


def kernel(nx, ny, nz, X, Y, mat_hbm, table_hbm, grad_hbm, out, mat, table, grad, eps, peer, halo, halo_peer, faces,
           zs, zd, zi, in_sem, table_sem, main_send, main_recv, face_send, face_recv, fwd_send, fwd_recv, entered):
    Z = mat.shape[-1]
    zpeers = 1 if nz == 2 else 2
    xs, ys = 2 * Y, 2 * X
    pieces = ((0, xs), (xs, xs), (2 * xs, ys), (2 * xs + ys, ys)) + tuple(
        (2 * xs + 2 * ys + 8 * c, 8) for c in range(4)
    )
    rows = X * Y // CHUNKS

    def load(c):
        part = pl.ds(c * rows, rows)
        return (
            pltpu.make_async_copy(mat_hbm.at[part], mat.at[part], in_sem.at[0, c]),
            pltpu.make_async_copy(grad_hbm.at[part], grad.at[part], in_sem.at[1, c]),
        )

    order = (0, CHUNKS - 1) + tuple(range(1, CHUNKS - 1))
    me = (lax.axis_index("gx"), lax.axis_index("gy"), lax.axis_index("gz"))
    sizes = (nx, ny, nz)

    def near(*steps):
        return tuple(
            me[k] if d == 0 else lax.rem(me[k] + (d + sizes[k]), sizes[k]) for k, d in enumerate(steps)
        )

    zdevs = [near(0, 0, 1), near(0, 0, -1)][:zpeers]
    xdevs = [near(-1, 0, 0), near(1, 0, 0)]
    around = [near(0, -1, 0), near(0, 1, 0)] + xdevs
    barrier = pltpu.get_barrier_semaphore()
    for dev in around + zdevs:
        pl.semaphore_signal(barrier, inc=1, device_id=dev, device_id_type=MESH)

    table_copy = pltpu.make_async_copy(table_hbm, table, table_sem)
    table_copy.start()
    for c in order:
        for copy in load(c):
            copy.start()

    table_copy.wait()
    values = [table[k] for k in range(table.shape[0])]

    def look(c):
        for copy in load(c):
            copy.wait()

        def plane(i, carry):
            part = pl.ds(pl.multiple_of(c * rows + i * Y, Y), Y)
            m = mat[part]
            v = jnp.full(m.shape, values[0], jnp.float32)
            for k in range(1, len(values)):
                v = jnp.where(m == k, values[k], v)
            eps[part] = v * grad[part].astype(jnp.float32)
            return carry

        lax.fori_loop(0, rows // Y, plane, 0)

    def main_copy(c, side):
        part = pl.ds(c * rows, rows)
        return pltpu.make_async_remote_copy(
            eps.at[part], peer.at[side, part], main_send.at[side, c], main_recv.at[side, c],
            device_id=zdevs[side], device_id_type=MESH,
        )

    def piece(ref, k):
        return ref.at[pl.ds(pieces[k][0], pieces[k][1])]

    def face_copy(k, src, dev):
        return pltpu.make_async_remote_copy(
            src, piece(halo, k), face_send.at[k], face_recv.at[k], device_id=dev, device_id_type=MESH
        )

    def forward(k, side):
        start, count = pieces[k]
        return pltpu.make_async_remote_copy(
            piece(halo, k), halo_peer.at[side, pl.ds(start, count)], fwd_send.at[side, k],
            fwd_recv.at[side, k], device_id=zdevs[side], device_id_type=MESH,
        )

    edges = 2 * ys
    copies = {
        1: face_copy(1, eps.at[pl.ds(0, xs)], near(-1, 0, 0)),
        0: face_copy(0, eps.at[pl.ds(X * Y - xs, xs)], near(1, 0, 0)),
        3: face_copy(3, faces.at[pl.ds(0, ys)], near(0, -1, 0)),
        2: face_copy(2, faces.at[pl.ds(ys, ys)], near(0, 1, 0)),
    }
    for sx in range(2):
        for sy in range(2):
            mine, theirs = 2 * sx + sy, 2 * (1 - sx) + (1 - sy)
            copies[4 + theirs] = face_copy(
                4 + theirs, faces.at[pl.ds(edges + 8 * mine, 8)], near(2 * sx - 1, 2 * sy - 1, 0)
            )
    mains = {(c, s): main_copy(c, s) for c in order for s in range(zpeers)}
    forwards = {(k, s): forward(k, s) for k in range(8) for s in range(zpeers)}

    for c in order:
        look(c)
    for l in range(2):
        for side in range(2):
            y = l if side == 0 else Y - 2 + l
            faces[pl.ds(side * ys + l * X, X)] = eps[pl.ds(y, X, stride=Y)]
    faces[pl.ds(edges, 32)] = jnp.ones((32, Z), jnp.float32)
    for sx in range(2):
        for sy in range(2):
            for a in range(2):
                x, y = (X - 2) * sx + a, (Y - 2) * sy
                faces[pl.ds(edges + 8 * (2 * sx + sy) + 2 * a, 2)] = eps[pl.ds(x * Y + y, 2)]
    pl.semaphore_wait(barrier, len(around) + len(zdevs))
    for dev in xdevs:
        pl.semaphore_signal(entered, inc=1, device_id=dev, device_id_type=MESH)
    for k in range(4):
        copies[k].start()
    for c in order:
        for s in range(zpeers):
            mains[c, s].start()

    def zfilter(e, low, high):
        lane = lax.broadcasted_iota(jnp.int32, e.shape, 1)
        m1 = pltpu.roll(jnp.where(lane == Z - 1, low, e), 1, 1)
        m2 = pltpu.roll(jnp.where(lane >= Z - 2, low, e), 2, 1)
        p1 = pltpu.roll(jnp.where(lane == 0, high, e), Z - 1, 1)
        p2 = pltpu.roll(jnp.where(lane < 2, high, e), Z - 2, 1)
        both, prod = m1 + p1, m1 * p1
        return e + both, (p1 - m1) + (p2 - m2), (prod + e * both) * inverse(e * prod)

    def sides(ref, part):
        low = ref[0, part]
        return low, (low if zpeers == 1 else ref[1, part])

    def arrive(ks):
        for k in ks:
            copies[k].wait_recv()
            for s in range(zpeers):
                forwards[k, s].start()

    for n, c in enumerate(order):
        for s in range(zpeers):
            mains[c, s].wait_recv()

        def plane(i, carry):
            x = c * (rows // Y) + i
            part = pl.ds(pl.multiple_of(x * Y, Y), Y)
            for ref, value in zip((zs, zd, zi), zfilter(eps[part], *sides(peer, part))):
                ref[x + 2, PAD:PAD + Y] = value
            return carry

        lax.fori_loop(0, rows // Y, plane, 0)
        if n == 0:
            pl.semaphore_wait(entered, len(xdevs))
            for k in range(4, 8):
                copies[k].start()
        elif n == 2:
            arrive((2, 3))
        elif n == 3:
            arrive((0, 1))

    def yrows(ref, p, j, shift):
        return ref[p, PAD + 16 * j + shift:PAD + 16 * j + shift + 16]

    def lead(p, j):
        a, b = yrows(zs, p, j, -1), yrows(zs, p, j, 1)
        return yrows(zs, p, j, 0) + (a + b)

    def rest(p, j):
        b = (yrows(zs, p, j, 1) - yrows(zs, p, j, -1)) + (yrows(zs, p, j, 2) - yrows(zs, p, j, -2))
        return b, sum(yrows(zd, p, j, k) for k in (-1, 0, 1)), sum(yrows(zi, p, j, k) for k in (-1, 0, 1))

    def outputs(j, start, count, unroll):
        def step(x, carry):
            (a0, a1, a2, a3), r0, r1 = carry
            a4 = lead(x + 4, j)
            r2 = rest(x + 3, j)
            total = a2 + (a1 + a3)
            gx = (a3 - a1) + (a4 - a0)
            gy, gz, inv = (u + v + w for u, v, w in zip(r0, r1, r2))
            den = gx * gx + gy * gy + gz * gz + 291.6
            q = inverse(total * den)
            recip = (den * q) * 27.0
            k = (inv * (1.0 / 27.0) - recip) * (total * q)
            kx, ky, kz = gx * k, gy * k, gz * k
            result = (gx * kx + recip, gy * ky + recip, gz * kz + recip, gx * ky, gx * kz, gy * kz)
            for n, value in enumerate(result):
                out[n, x, 16 * j:16 * j + 16] = value.astype(out.dtype)
            return (a1, a2, a3, a4), r1, r2

        carry = (tuple(lead(start + k, j) for k in range(4)), rest(start + 1, j), rest(start + 2, j))
        if count == unroll:
            for k in range(count):
                carry = step(start + k, carry)
        else:
            def block(i, carry):
                for k in range(unroll):
                    carry = step(start + i * unroll + k, carry)
                return carry

            lax.fori_loop(0, count // unroll, block, carry)

    def halo_filter(k):
        for s in range(zpeers):
            forwards[k, s].wait_recv()
        part = pl.ds(*pieces[k])
        fields = zfilter(halo[part], *sides(halo_peer, part))
        for ref, value in zip((zs, zd, zi), fields):
            if k < 2:
                p = k * (X + 2)
                ref[p, PAD:PAD + Y] = value[:Y]
                ref[p + 1, PAD:PAD + Y] = value[Y:]
            elif k < 4:
                flat = ref.reshape((X + 4) * (Y + 2 * PAD), Z)
                y = PAD - 2 if k == 2 else PAD + Y
                for l in range(2):
                    flat[pl.ds(2 * (Y + 2 * PAD) + y + l, X, stride=Y + 2 * PAD)] = value[l * X:(l + 1) * X]
            else:
                sx, sy = divmod(k - 4, 2)
                y = PAD - 2 if sy == 0 else PAD + Y
                for a in range(2):
                    ref[sx * (X + 2) + a, y:y + 2] = value[2 * a:2 * a + 2]

    pairs = Y // 16
    unroll = 4
    inside = range(1, pairs - 1)
    for j in inside:
        outputs(j, 2, X - 4, unroll)
    arrive(range(4, 8))
    halo_filter(2)
    halo_filter(3)
    outputs(0, 2, X - 4, unroll)
    outputs(pairs - 1, 2, X - 4, unroll)
    halo_filter(0)
    halo_filter(1)
    for j in inside:
        outputs(j, 0, 2, 2)
        outputs(j, X - 2, 2, 2)
    for k in range(4, 8):
        halo_filter(k)
    for j in (0, pairs - 1):
        outputs(j, 0, 2, 2)
        outputs(j, X - 2, 2, 2)
    for copy in list(copies.values()) + list(mains.values()) + list(forwards.values()):
        copy.wait_send()


def write_out(result, out, sem):
    copies = [pltpu.make_async_copy(result.at[n], out.at[n], sem.at[n]) for n in range(out.shape[0])]
    for copy in copies:
        copy.start()
    for copy in copies:
        copy.wait()


def solution(mesh):
    nx, ny, nz = mesh.shape["gx"], mesh.shape["gy"], mesh.shape["gz"]

    def local(material, eps_table, grading):
        X, Y, Z = material.shape
        zpeers = 1 if nz == 2 else 2
        halo_rows = 4 * Y + 4 * X + 32
        any_space = pl.BlockSpec(memory_space=pl.ANY)
        dma = pltpu.SemaphoreType.DMA
        field = pltpu.VMEM((X + 4, Y + 2 * PAD, Z), jnp.float32)
        result = pl.pallas_call(
            functools.partial(kernel, nx, ny, nz, X, Y),
            out_shape=pltpu.VMEM((6, X, Y, Z), jnp.bfloat16),
            in_specs=[pl.BlockSpec(memory_space=pltpu.HBM)] * 3,
            out_specs=pl.BlockSpec(memory_space=pltpu.VMEM),
            scratch_shapes=[
                pltpu.VMEM((X * Y, Z), jnp.int32),
                pltpu.SMEM(eps_table.shape, jnp.float32),
                pltpu.VMEM((X * Y, Z), jnp.bfloat16),
                pltpu.VMEM((X * Y, Z), jnp.float32),
                pltpu.VMEM((zpeers, X * Y, Z), jnp.float32),
                pltpu.VMEM((halo_rows, Z), jnp.float32),
                pltpu.VMEM((zpeers, halo_rows, Z), jnp.float32),
                pltpu.VMEM((4 * X + 32, Z), jnp.float32),
                field, field, field,
                dma((2, CHUNKS)), dma(()),
                dma((zpeers, CHUNKS)), dma((zpeers, CHUNKS)),
                dma((8,)), dma((8,)),
                dma((zpeers, 8)), dma((zpeers, 8)),
                pltpu.SemaphoreType.REGULAR,
            ],
            compiler_params=pltpu.CompilerParams(
                collective_id=0, has_side_effects=True, vmem_limit_bytes=24 * 2**20
            ),
        )(*(pltpu.with_memory_space_constraint(a, pltpu.HBM)
            for a in (material.reshape(X * Y, Z), eps_table, grading.reshape(X * Y, Z))))
        return pl.pallas_call(
            write_out,
            out_shape=jax.ShapeDtypeStruct((6, X, Y, Z), jnp.bfloat16),
            in_specs=[pl.BlockSpec(memory_space=pltpu.VMEM)],
            out_specs=any_space,
            scratch_shapes=[dma((6,))],
            compiler_params=pltpu.CompilerParams(vmem_limit_bytes=24 * 2**20),
        )(result)

    return jax.shard_map(
        local,
        mesh=mesh,
        in_specs=(P("gx", "gy", "gz"), P(), P("gx", "gy", "gz")),
        out_specs=P(None, "gx", "gy", "gz"),
        check_vma=False,
    )
```

```python
import functools

import jax
import jax.numpy as jnp
from jax import lax
from jax.experimental import pallas as pl
from jax.experimental.pallas import tpu as pltpu
from jax.sharding import PartitionSpec as P

MESH = pl.DeviceIdType.MESH
CHUNKS = 4
PAD = 8


def inverse(x):
    guess = pl.reciprocal(x, approx=True)
    return guess * (2.0 - x * guess)


def yrows(ref, p, j, shift):
    return ref[p, PAD + 16 * j + shift:PAD + 16 * j + shift + 16]


def lead(fields, p, j):
    zs = fields[0]
    a, b = yrows(zs, p, j, -1), yrows(zs, p, j, 1)
    return yrows(zs, p, j, 0) + (a + b)


def rest(fields, p, j):
    zs, zd, zi = fields
    b = (yrows(zs, p, j, 1) - yrows(zs, p, j, -1)) + (yrows(zs, p, j, 2) - yrows(zs, p, j, -2))
    return b, sum(yrows(zd, p, j, k) for k in (-1, 0, 1)), sum(yrows(zi, p, j, k) for k in (-1, 0, 1))


def outputs(fields, put, j, start, count, unroll):
    def step(x, carry):
        (a0, a1, a2, a3), r0, r1 = carry
        a4 = lead(fields, x + 4, j)
        r2 = rest(fields, x + 3, j)
        total = a2 + (a1 + a3)
        gx = (a3 - a1) + (a4 - a0)
        gy, gz, inv = (u + v + w for u, v, w in zip(r0, r1, r2))
        den = gx * gx + gy * gy + gz * gz + 291.6
        q = inverse(total * den)
        recip = (den * q) * 27.0
        k = (inv * (1.0 / 27.0) - recip) * (total * q)
        kx, ky, kz = gx * k, gy * k, gz * k
        result = (gx * kx + recip, gy * ky + recip, gz * kz + recip, gx * ky, gx * kz, gy * kz)
        for n, value in enumerate(result):
            put(n, x, j, value)
        return (a1, a2, a3, a4), r1, r2

    carry = (tuple(lead(fields, start + k, j) for k in range(4)), rest(fields, start + 1, j), rest(fields, start + 2, j))
    if count == unroll:
        for k in range(count):
            carry = step(start + k, carry)
    else:
        def block(i, carry):
            for k in range(unroll):
                carry = step(start + i * unroll + k, carry)
            return carry

        lax.fori_loop(0, count // unroll, block, carry)


def kernel(nx, ny, nz, X, Y, mat_hbm, table_hbm, grad_hbm, out, zs, zd, zi, mat, table, grad, eps, peer,
           halo, halo_peer, faces, in_sem, table_sem, main_send, main_recv, face_send, face_recv, fwd_send, fwd_recv, entered):
    Z = mat.shape[-1]
    zpeers = 1 if nz == 2 else 2
    xs, ys = 2 * Y, 2 * X
    pieces = ((0, xs), (xs, xs), (2 * xs, ys), (2 * xs + ys, ys)) + tuple(
        (2 * xs + 2 * ys + 8 * c, 8) for c in range(4)
    )
    rows = X * Y // CHUNKS

    def load(c):
        part = pl.ds(c * rows, rows)
        return (
            pltpu.make_async_copy(mat_hbm.at[part], mat.at[part], in_sem.at[0, c]),
            pltpu.make_async_copy(grad_hbm.at[part], grad.at[part], in_sem.at[1, c]),
        )

    order = (0, CHUNKS - 1) + tuple(range(1, CHUNKS - 1))
    me = (lax.axis_index("gx"), lax.axis_index("gy"), lax.axis_index("gz"))
    sizes = (nx, ny, nz)

    def near(*steps):
        return tuple(
            me[k] if d == 0 else lax.rem(me[k] + (d + sizes[k]), sizes[k]) for k, d in enumerate(steps)
        )

    zdevs = [near(0, 0, 1), near(0, 0, -1)][:zpeers]
    xdevs = [near(-1, 0, 0), near(1, 0, 0)]
    around = [near(0, -1, 0), near(0, 1, 0)] + xdevs
    barrier = pltpu.get_barrier_semaphore()
    for dev in around + zdevs:
        pl.semaphore_signal(barrier, inc=1, device_id=dev, device_id_type=MESH)

    table_copy = pltpu.make_async_copy(table_hbm, table, table_sem)
    table_copy.start()
    for c in order:
        for copy in load(c):
            copy.start()

    table_copy.wait()
    values = [table[k] for k in range(table.shape[0])]

    def look(c):
        for copy in load(c):
            copy.wait()

        def plane(i, carry):
            part = pl.ds(pl.multiple_of(c * rows + i * Y, Y), Y)
            m = mat[part]
            v = jnp.full(m.shape, values[0], jnp.float32)
            for k in range(1, len(values)):
                v = jnp.where(m == k, values[k], v)
            eps[part] = v * grad[part].astype(jnp.float32)
            return carry

        lax.fori_loop(0, rows // Y, plane, 0)

    def main_copy(c, side):
        part = pl.ds(c * rows, rows)
        return pltpu.make_async_remote_copy(
            eps.at[part], peer.at[side, part], main_send.at[side, c], main_recv.at[side, c],
            device_id=zdevs[side], device_id_type=MESH,
        )

    def piece(ref, k):
        return ref.at[pl.ds(pieces[k][0], pieces[k][1])]

    def face_copy(k, src, dev):
        return pltpu.make_async_remote_copy(
            src, piece(halo, k), face_send.at[k], face_recv.at[k], device_id=dev, device_id_type=MESH
        )

    def forward(k, side):
        start, count = pieces[k]
        return pltpu.make_async_remote_copy(
            piece(halo, k), halo_peer.at[side, pl.ds(start, count)], fwd_send.at[side, k],
            fwd_recv.at[side, k], device_id=zdevs[side], device_id_type=MESH,
        )

    edges = 2 * ys
    copies = {
        1: face_copy(1, eps.at[pl.ds(0, xs)], near(-1, 0, 0)),
        0: face_copy(0, eps.at[pl.ds(X * Y - xs, xs)], near(1, 0, 0)),
        3: face_copy(3, faces.at[pl.ds(0, ys)], near(0, -1, 0)),
        2: face_copy(2, faces.at[pl.ds(ys, ys)], near(0, 1, 0)),
    }
    for sx in range(2):
        for sy in range(2):
            mine, theirs = 2 * sx + sy, 2 * (1 - sx) + (1 - sy)
            copies[4 + theirs] = face_copy(
                4 + theirs, faces.at[pl.ds(edges + 8 * mine, 8)], near(2 * sx - 1, 2 * sy - 1, 0)
            )
    mains = {(c, s): main_copy(c, s) for c in order for s in range(zpeers)}
    forwards = {(k, s): forward(k, s) for k in range(8) for s in range(zpeers)}

    for c in order:
        look(c)
    for l in range(2):
        for side in range(2):
            y = l if side == 0 else Y - 2 + l
            faces[pl.ds(side * ys + l * X, X)] = eps[pl.ds(y, X, stride=Y)]
    faces[pl.ds(edges, 32)] = jnp.ones((32, Z), jnp.float32)
    for sx in range(2):
        for sy in range(2):
            for a in range(2):
                x, y = (X - 2) * sx + a, (Y - 2) * sy
                faces[pl.ds(edges + 8 * (2 * sx + sy) + 2 * a, 2)] = eps[pl.ds(x * Y + y, 2)]
    pl.semaphore_wait(barrier, len(around) + len(zdevs))
    for dev in xdevs:
        pl.semaphore_signal(entered, inc=1, device_id=dev, device_id_type=MESH)
    for k in range(4):
        copies[k].start()
    for c in order:
        for s in range(zpeers):
            mains[c, s].start()

    def zfilter(e, low, high):
        lane = lax.broadcasted_iota(jnp.int32, e.shape, 1)
        m1 = pltpu.roll(jnp.where(lane == Z - 1, low, e), 1, 1)
        m2 = pltpu.roll(jnp.where(lane >= Z - 2, low, e), 2, 1)
        p1 = pltpu.roll(jnp.where(lane == 0, high, e), Z - 1, 1)
        p2 = pltpu.roll(jnp.where(lane < 2, high, e), Z - 2, 1)
        both, prod = m1 + p1, m1 * p1
        return e + both, (p1 - m1) + (p2 - m2), (prod + e * both) * inverse(e * prod)

    def sides(ref, part):
        low = ref[0, part]
        return low, (low if zpeers == 1 else ref[1, part])

    def arrive(ks):
        for k in ks:
            copies[k].wait_recv()
            for s in range(zpeers):
                forwards[k, s].start()

    for n, c in enumerate(order):
        for s in range(zpeers):
            mains[c, s].wait_recv()

        def plane(i, carry):
            x = c * (rows // Y) + i
            part = pl.ds(pl.multiple_of(x * Y, Y), Y)
            for ref, value in zip((zs, zd, zi), zfilter(eps[part], *sides(peer, part))):
                ref[x + 2, PAD:PAD + Y] = value
            return carry

        lax.fori_loop(0, rows // Y, plane, 0)
        if n == 0:
            pl.semaphore_wait(entered, len(xdevs))
            for k in range(4, 8):
                copies[k].start()
        elif n == 2:
            arrive((2, 3))
        elif n == 3:
            arrive((0, 1))

    def halo_filter(k):
        for s in range(zpeers):
            forwards[k, s].wait_recv()
        part = pl.ds(*pieces[k])
        fields = zfilter(halo[part], *sides(halo_peer, part))
        for ref, value in zip((zs, zd, zi), fields):
            if k < 2:
                p = k * (X + 2)
                ref[p, PAD:PAD + Y] = value[:Y]
                ref[p + 1, PAD:PAD + Y] = value[Y:]
            elif k < 4:
                flat = ref.reshape((X + 4) * (Y + 2 * PAD), Z)
                y = PAD - 2 if k == 2 else PAD + Y
                for l in range(2):
                    flat[pl.ds(2 * (Y + 2 * PAD) + y + l, X, stride=Y + 2 * PAD)] = value[l * X:(l + 1) * X]
            else:
                sx, sy = divmod(k - 4, 2)
                y = PAD - 2 if sy == 0 else PAD + Y
                for a in range(2):
                    ref[sx * (X + 2) + a, y:y + 2] = value[2 * a:2 * a + 2]

    pairs = Y // 16
    unroll = 4
    inside = range(1, pairs - 1)
    fields = (zs, zd, zi)

    def put(n, x, j, value):
        out[n, x, 16 * j:16 * j + 16] = value.astype(out.dtype)

    for j in inside:
        outputs(fields, put, j, 2, X - 4, unroll)
    halo_filter(2)
    halo_filter(3)
    outputs(fields, put, 0, 2, X - 4, unroll)
    arrive(range(4, 8))
    outputs(fields, put, pairs - 1, 2, X - 4, unroll)
    for k in (0, 1, 4, 5, 6, 7):
        halo_filter(k)
    for copy in list(copies.values()) + list(mains.values()) + list(forwards.values()):
        copy.wait_send()


def write_out(result, zs, zd, zi, out, ends, sem, end_sem):
    _, X, Y, _ = out.shape
    inner = pl.ds(2, X - 4)
    copies = [
        pltpu.make_async_copy(result.at[n, inner], out.at[n, inner], sem.at[n]) for n in range(out.shape[0])
    ]
    for copy in copies:
        copy.start()
    for side in range(2):
        start = side * (X - 2)

        def put(n, x, j, value):
            ends[side, n, x - start, 16 * j:16 * j + 16] = value.astype(out.dtype)

        for j in range(Y // 16):
            outputs((zs, zd, zi), put, j, start, 2, 2)
        tail = [
            pltpu.make_async_copy(ends.at[side, n], out.at[n, pl.ds(start, 2)], end_sem.at[side, n])
            for n in range(out.shape[0])
        ]
        for copy in tail:
            copy.start()
        copies += tail
    for copy in copies:
        copy.wait()


def solution(mesh):
    nx, ny, nz = mesh.shape["gx"], mesh.shape["gy"], mesh.shape["gz"]

    def local(material, eps_table, grading):
        X, Y, Z = material.shape
        zpeers = 1 if nz == 2 else 2
        halo_rows = 4 * Y + 4 * X + 32
        any_space = pl.BlockSpec(memory_space=pl.ANY)
        dma = pltpu.SemaphoreType.DMA
        vmem = pl.BlockSpec(memory_space=pltpu.VMEM)
        field = pltpu.VMEM((X + 4, Y + 2 * PAD, Z), jnp.float32)
        result = pl.pallas_call(
            functools.partial(kernel, nx, ny, nz, X, Y),
            out_shape=(pltpu.VMEM((6, X, Y, Z), jnp.bfloat16), field, field, field),
            in_specs=[pl.BlockSpec(memory_space=pltpu.HBM)] * 3,
            out_specs=(vmem,) * 4,
            scratch_shapes=[
                pltpu.VMEM((X * Y, Z), jnp.int32),
                pltpu.SMEM(eps_table.shape, jnp.float32),
                pltpu.VMEM((X * Y, Z), jnp.bfloat16),
                pltpu.VMEM((X * Y, Z), jnp.float32),
                pltpu.VMEM((zpeers, X * Y, Z), jnp.float32),
                pltpu.VMEM((halo_rows, Z), jnp.float32),
                pltpu.VMEM((zpeers, halo_rows, Z), jnp.float32),
                pltpu.VMEM((4 * X + 32, Z), jnp.float32),
                dma((2, CHUNKS)), dma(()),
                dma((zpeers, CHUNKS)), dma((zpeers, CHUNKS)),
                dma((8,)), dma((8,)),
                dma((zpeers, 8)), dma((zpeers, 8)),
                pltpu.SemaphoreType.REGULAR,
            ],
            compiler_params=pltpu.CompilerParams(
                collective_id=0, has_side_effects=True, vmem_limit_bytes=24 * 2**20
            ),
        )(*(pltpu.with_memory_space_constraint(a, pltpu.HBM)
            for a in (material.reshape(X * Y, Z), eps_table, grading.reshape(X * Y, Z))))
        return pl.pallas_call(
            write_out,
            out_shape=jax.ShapeDtypeStruct((6, X, Y, Z), jnp.bfloat16),
            in_specs=[vmem] * 4,
            out_specs=any_space,
            scratch_shapes=[pltpu.VMEM((2, 6, 2, Y, Z), jnp.bfloat16), dma((6,)), dma((2, 6))],
            compiler_params=pltpu.CompilerParams(vmem_limit_bytes=24 * 2**20),
        )(*result)

    return jax.shard_map(
        local,
        mesh=mesh,
        in_specs=(P("gx", "gy", "gz"), P(), P("gx", "gy", "gz")),
        out_specs=P(None, "gx", "gy", "gz"),
        check_vma=False,
    )
```
